32 devices in a mesh: rows: 8 (over y, x, core), feat: 4 (over z).
Axes of the slice: x: 2, y: 2, z: 4, core: 2. Of those that a mesh axis runs over, the one named last changes fastest.
Arguments:
- bins: int32 [8192, 512], P('rows', 'feat'), may hold values from -2147483648 to 2147483647, as said below
- hessian: float32 [32768], P('rows'), may hold values from 0.05 to 1
- thresholds: float32 [128], replicated, may hold values from 0.02 to 0.98
Outputs:
- cuts: float32 [512, 128], P('feat')
The draws below stay inside these ranges and needn't reach their ends.
Inputs may be any that keep to these rules, and one draw needn't show every extreme that they name: `bins`: each word holds the bin ids, 0 to 255, of rows 4i to 4i + 3 of one feature, row 4i + k in bits 8k to 8k + 7 of the two's complement word.
All inputs are finite; a program needn't handle non-finite values.
Results may differ from the reference program's by a relative error of at most 0.000065.
Values sent between devices are 32-bit elements; how exact they have to be, the bound alone decides.
A program may use at most 192 MiB of HBM per device.

```python
import math
import jax
import jax.numpy as jnp

F = 512
BINS = 256
Q = 128
ROW_DEV = 4096
ROWS = 32768
N_ROWS = 8


def draw_bins(key, part):
    key = jax.random.fold_in(key, 17)
    first, second, third, fourth = jax.random.split(key, 4)
    spread = jax.random.randint(first, (ROWS, F), 0, BINS)
    centers = jax.random.randint(second, (N_ROWS, F), 0, BINS)
    offsets = jax.random.randint(third, (ROWS, F), 0, 8)
    banded = jax.random.randint(fourth, (ROWS, F), 0, 2) == 0
    owner = jnp.arange(ROWS, dtype=jnp.int32) // ROW_DEV
    center_rows = centers[owner]
    ids = jnp.where(banded, (center_rows + offsets) % BINS, spread).astype(jnp.int32)
    grouped = ids.reshape(ROWS // 4, 4, F)
    packed = jnp.zeros((ROWS // 4, F), jnp.int32)
    for k in range(4):
        packed = jnp.bitwise_or(packed, jnp.left_shift(grouped[:, k, :], 8 * k))
    return packed.astype(jnp.int32)


def block_levels(own_key, dims, pieces, least, largest):
    loudness = 1.0
    for dim, shards_of in pieces:
        heights = jax.random.uniform(jax.random.fold_in(jax.random.fold_in(own_key, 6), dim), (shards_of,), jnp.float32, least / len(pieces), largest / len(pieces))
        loudness = loudness * jnp.repeat(jnp.exp(heights), dims[dim] // shards_of).reshape((-1,) + (1,) * (len(dims) - 1 - dim))
    return loudness


def setup_inputs(seed: int = 0) -> dict:
    key_list = jax.random.split(jax.random.key(seed), 4)
    return {
        "bins": draw_bins(jax.random.fold_in(key_list[3], 71), 0),
        "hessian": jnp.clip(jnp.exp(math.log(1.0) - 2.9957323 * jax.random.uniform(key_list[1], (ROWS,), jnp.float32) ** block_levels(key_list[1], (ROWS,), ((0, 8),), -0.2, 0.2)), 0.05, 1.0),
        "thresholds": jnp.clip(jax.random.uniform(key_list[2], (Q,), jnp.float32, 0.02, 0.98), 0.02, 0.98),
    }


def unpack(words):
    parts = [jnp.bitwise_and(jnp.right_shift(words, 8 * k), 255) for k in range(4)]
    stacked = jnp.stack(parts, axis=1)
    return stacked.reshape(words.shape[0] * 4, words.shape[1]).astype(jnp.int32)


def cut_positions(hist, thresholds):
    cum = jnp.cumsum(hist, axis=1)
    before = cum - hist
    total = cum[:, -1]
    target = thresholds[None, :, None] * total[:, None, None]
    ratio = (target - before[:, None, :]) / (hist[:, None, :] + 1.0)
    return jnp.sum(jnp.clip(ratio, 0.0, 1.0), axis=2)


def reference(bins, hessian, thresholds):
    ids = unpack(bins)

    def one_feature(column):
        return jax.ops.segment_sum(hessian, column, num_segments=BINS)

    hist = jax.vmap(one_feature)(ids.T).astype(jnp.float32)
    return cut_positions(hist, thresholds)
```

```python
import functools

import jax
import jax.numpy as jnp
from jax import lax
from jax.experimental import pallas as pl
from jax.experimental.pallas import tpu as pltpu
from jax.sharding import PartitionSpec as P

BINS = 256
LEVELS = 16
GROUP = 16
LANES = 128
CHUNK = 256
MESH = pl.DeviceIdType.MESH


def kernel(ranks, bins_ref, hess_ref, thr_ref, out_ref, cols, wts, stage, inbox, mine, send_sem, recv_sem, gather_send, gather_recv):
    words, width = bins_ref.shape
    groups = width // GROUP
    replicas = ranks // groups
    lanes = LEVELS * GROUP
    me = lax.axis_index("rows")
    team, seat = me // groups, me % groups

    barrier = pltpu.get_barrier_semaphore()
    for step in range(1, ranks):
        pl.semaphore_signal(barrier, inc=1, device_id={"rows": (me + step) % ranks}, device_id_type=MESH)

    span = 4 * LANES
    tiles = words // LANES
    flat = jnp.concatenate([hess_ref[pl.ds(j, tiles, stride=4), :] for j in range(4)], axis=1)
    top = flat.astype(jnp.bfloat16).astype(jnp.float32)
    rest = flat - top
    row = lax.broadcasted_iota(jnp.int32, (span, span), 0)
    col = lax.broadcasted_iota(jnp.int32, (span, span), 1)
    order = jnp.where(row == 4 * (col % LANES) + col // LANES, 1.0, 0.0).astype(jnp.bfloat16)
    pieces = jnp.concatenate([top, rest], axis=0).astype(jnp.bfloat16)
    moved = jnp.dot(pieces, order, preferred_element_type=jnp.float32)
    for piece in range(2):
        for k in range(4):
            for t in range(tiles):
                line = moved[piece * tiles + t : piece * tiles + t + 1, k * LANES : (k + 1) * LANES]
                wts[piece, k, :, t * LANES : (t + 1) * LANES] = jnp.broadcast_to(line, (GROUP, LANES)).astype(jnp.bfloat16)

    for t in range(tiles):
        cols[:, t * LANES : (t + 1) * LANES] = bins_ref[t * LANES : (t + 1) * LANES, :].T

    def group_hist(group):
        base = pl.multiple_of(group * GROUP, GROUP)
        zero = jnp.zeros((GROUP, CHUNK), jnp.bfloat16)
        one = jnp.ones((GROUP, CHUNK), jnp.bfloat16)
        sums = [None, None]
        index = 0
        for c in range(words // CHUNK):
            part = cols[pl.ds(base, GROUP), c * CHUNK : (c + 1) * CHUNK]
            for k in range(4):
                high = jnp.bitwise_and(jnp.right_shift(part, 8 * k + 4), 15).astype(jnp.float32).astype(jnp.bfloat16)
                low = jnp.bitwise_and(jnp.right_shift(part, 8 * k), 15).astype(jnp.float32).astype(jnp.bfloat16)
                w0 = wts[0, k, :, c * CHUNK : (c + 1) * CHUNK]
                w1 = wts[1, k, :, c * CHUNK : (c + 1) * CHUNK]
                hot = [high == jnp.bfloat16(h) for h in range(LEVELS)]
                left = jnp.concatenate([jnp.where(m, w0, zero) for m in hot] + [jnp.where(m, w1, zero) for m in hot], axis=0)
                right = jnp.concatenate([jnp.where(low == jnp.bfloat16(l), one, zero) for l in range(LEVELS)], axis=0)
                part_sum = lax.dot_general(left, right, (((1,), (1,)), ((), ())), preferred_element_type=jnp.float32)
                side = index % 2
                sums[side] = part_sum if sums[side] is None else sums[side] + part_sum
                index += 1
        both = sums[0] + sums[1]
        joint = both[:lanes] + both[lanes:]
        own_row = lax.broadcasted_iota(jnp.int32, (GROUP, lanes), 0)
        own_col = lax.broadcasted_iota(jnp.int32, (GROUP, lanes), 1)
        keep = own_row == own_col % GROUP
        lines = []
        for h in range(LEVELS):
            lines.append(jnp.sum(jnp.where(keep, joint[h * GROUP : (h + 1) * GROUP], 0.0), axis=0, keepdims=True))
        return jnp.concatenate(lines, axis=0)

    def outgoing(step, e):
        target = ((team + e) % replicas) * groups + (seat + step) % groups
        slot = step * replicas + e
        return pltpu.make_async_remote_copy(
            src_ref=stage.at[step],
            dst_ref=inbox.at[slot],
            send_sem=send_sem.at[slot],
            recv_sem=recv_sem.at[slot],
            device_id={"rows": target},
            device_id_type=MESH,
        )

    def do_group(turn, carry):
        step = (turn + 1) % groups
        stage[step] = group_hist((seat + step) % groups)

        @pl.when(turn == 0)
        def _():
            pl.semaphore_wait(barrier, ranks - 1)

        @pl.when(turn < groups - 1)
        def _():
            for e in range(replicas):
                outgoing(step, e).start()

        return carry

    lax.fori_loop(0, groups, do_group, 0)
    for e in range(1, replicas):
        outgoing(0, e).start()

    total = stage[0]
    for step in range(groups):
        for e in range(replicas):
            if step + e > 0:
                outgoing(step, e).wait()
                total = total + inbox[step * replicas + e]

    src = lax.broadcasted_iota(jnp.int32, (lanes, lanes), 0)
    dst = lax.broadcasted_iota(jnp.int32, (lanes, lanes), 1)
    same = src % GROUP == dst % GROUP
    earlier = jnp.where(jnp.logical_and(same, src < dst), 1.0, 0.0).astype(jnp.bfloat16)
    every = jnp.where(same, 1.0, 0.0).astype(jnp.bfloat16)
    p0 = total.astype(jnp.bfloat16).astype(jnp.float32)
    p1 = (total - p0).astype(jnp.bfloat16).astype(jnp.float32)
    p2 = total - p0 - p1
    split = jnp.concatenate([p0, p1, p2], axis=0).astype(jnp.bfloat16)
    inner3 = jnp.dot(split, earlier, preferred_element_type=jnp.float32)
    level3 = jnp.dot(split, every, preferred_element_type=jnp.float32)
    inner = inner3[:LEVELS] + inner3[LEVELS : 2 * LEVELS] + inner3[2 * LEVELS :]
    level = level3[:LEVELS] + level3[LEVELS : 2 * LEVELS] + level3[2 * LEVELS :]
    inv = 1.0 / (total + 1.0)
    column = jnp.broadcast_to(thr_ref[...], (LANES, thr_ref.shape[1])).T
    whole = jnp.sum(level, axis=0, keepdims=True)
    target = column * whole[:, :LANES]
    run = jnp.zeros((1, lanes), jnp.float32)
    acc = jnp.zeros((thr_ref.shape[1], LANES), jnp.float32)
    for h in range(LEVELS):
        before = inner[h : h + 1] + run
        run = run + level[h : h + 1]
        for t in range(lanes // LANES):
            cut = slice(t * LANES, (t + 1) * LANES)
            ratio = (target - before[:, cut]) * inv[h : h + 1, cut]
            acc = acc + jnp.clip(ratio, 0.0, 1.0)
    turned = acc.T
    cuts = turned[:GROUP]
    for j in range(1, LANES // GROUP):
        cuts = cuts + turned[j * GROUP : (j + 1) * GROUP]
    mine[...] = cuts
    here = pl.multiple_of(seat * GROUP, GROUP)

    def spread(step):
        return pltpu.make_async_remote_copy(
            src_ref=mine,
            dst_ref=out_ref.at[pl.ds(here, GROUP), :],
            send_sem=gather_send.at[step],
            recv_sem=gather_recv.at[step],
            device_id={"rows": team * groups + (seat + step) % groups},
            device_id_type=MESH,
        )

    for step in range(1, groups):
        spread(step).start()
    out_ref[pl.ds(here, GROUP), :] = cuts
    for step in range(1, groups):
        spread(step).wait()


def solution(mesh):
    ranks = mesh.shape["rows"]

    def local(bins, hessian, thresholds):
        words, width = bins.shape
        groups = width // GROUP
        quantiles = thresholds.shape[0]
        lanes = LEVELS * GROUP
        return pl.pallas_call(
            functools.partial(kernel, ranks),
            out_shape=jax.ShapeDtypeStruct((width, quantiles), jnp.float32),
            in_specs=[pl.BlockSpec(memory_space=pltpu.VMEM)] * 3,
            out_specs=pl.BlockSpec(memory_space=pltpu.VMEM),
            scratch_shapes=[
                pltpu.VMEM((width, words), jnp.int32),
                pltpu.VMEM((2, 4, GROUP, words), jnp.bfloat16),
                pltpu.VMEM((groups, LEVELS, lanes), jnp.float32),
                pltpu.VMEM((ranks, LEVELS, lanes), jnp.float32),
                pltpu.VMEM((GROUP, quantiles), jnp.float32),
                pltpu.SemaphoreType.DMA((ranks,)),
                pltpu.SemaphoreType.DMA((ranks,)),
                pltpu.SemaphoreType.DMA((groups,)),
                pltpu.SemaphoreType.DMA((groups,)),
            ],
            compiler_params=pltpu.CompilerParams(collective_id=0, has_side_effects=True),
        )(bins, hessian.reshape(-1, LANES), thresholds.reshape(1, -1))

    in_specs = (P("rows", "feat"), P("rows"), P())
    return jax.shard_map(local, mesh=mesh, in_specs=in_specs, out_specs=P("feat", None), check_vma=False)
```

```python
import functools

import jax
import jax.numpy as jnp
from jax import lax
from jax.experimental import pallas as pl
from jax.experimental.pallas import tpu as pltpu
from jax.sharding import PartitionSpec as P

BINS = 256
LEVELS = 16
GROUP = 16
LANES = 128
CHUNK = 256
MESH = pl.DeviceIdType.MESH


def kernel(ranks, bins_hbm, hess_hbm, thr_hbm, out_ref, bins_ref, hess_ref, thr_ref, cols, wts, stage, inbox, mine, load_sem, send_sem, recv_sem, gather_send, gather_recv):
    words, width = bins_ref.shape
    tiles = words // LANES
    hess_load = pltpu.make_async_copy(hess_hbm, hess_ref, load_sem.at[tiles])
    hess_load.start()
    bins_loads = []
    for t in range(tiles):
        part = pl.ds(t * LANES, LANES)
        bins_loads.append(pltpu.make_async_copy(bins_hbm.at[part, :], bins_ref.at[part, :], load_sem.at[t]))
        bins_loads[t].start()
    thr_load = pltpu.make_async_copy(thr_hbm, thr_ref, load_sem.at[tiles + 1])
    thr_load.start()
    groups = width // GROUP
    replicas = ranks // groups
    lanes = LEVELS * GROUP
    me = lax.axis_index("rows")
    team, seat = me // groups, me % groups

    barrier = pltpu.get_barrier_semaphore()
    for step in range(1, ranks):
        pl.semaphore_signal(barrier, inc=1, device_id={"rows": (me + step) % ranks}, device_id_type=MESH)

    span = 4 * LANES
    row = lax.broadcasted_iota(jnp.int32, (span, span), 0)
    col = lax.broadcasted_iota(jnp.int32, (span, span), 1)
    order = jnp.where(row == 4 * (col % LANES) + col // LANES, 1.0, 0.0).astype(jnp.bfloat16)
    hess_load.wait()
    flat = jnp.concatenate([hess_ref[pl.ds(j, tiles, stride=4), :] for j in range(4)], axis=1)
    right_factor = flat.astype(jnp.bfloat16).astype(jnp.float32)
    left_factor = jnp.ones_like(flat)
    miss = jnp.abs(flat - right_factor)
    for j in range(1, 128, 2):
        factor = 1.0 + j / 128.0
        other = (flat * (1.0 / factor)).astype(jnp.bfloat16).astype(jnp.float32)
        away = jnp.abs(flat - other * factor)
        better = away < miss
        left_factor = jnp.where(better, factor, left_factor)
        right_factor = jnp.where(better, other, right_factor)
        miss = jnp.minimum(miss, away)
    pieces = jnp.concatenate([left_factor, right_factor], axis=0).astype(jnp.bfloat16)
    moved = jnp.dot(pieces, order, preferred_element_type=jnp.float32)
    for piece in range(2):
        for k in range(4):
            for t in range(tiles):
                line = moved[piece * tiles + t : piece * tiles + t + 1, k * LANES : (k + 1) * LANES]
                wts[piece, k, :, t * LANES : (t + 1) * LANES] = jnp.broadcast_to(line, (GROUP, LANES)).astype(jnp.bfloat16)

    for t in range(tiles):
        bins_loads[t].wait()
        cols[:, t * LANES : (t + 1) * LANES] = bins_ref[t * LANES : (t + 1) * LANES, :].T

    def group_hist(group):
        base = pl.multiple_of(group * GROUP, GROUP)
        zero = jnp.zeros((GROUP, CHUNK), jnp.bfloat16)
        sums = [None, None]
        index = 0
        for c in range(words // CHUNK):
            part = cols[pl.ds(base, GROUP), c * CHUNK : (c + 1) * CHUNK]
            for k in range(4):
                high = jnp.bitwise_and(jnp.right_shift(part, 8 * k + 4), 15).astype(jnp.float32).astype(jnp.bfloat16)
                low = jnp.bitwise_and(jnp.right_shift(part, 8 * k), 15).astype(jnp.float32).astype(jnp.bfloat16)
                w0 = wts[0, k, :, c * CHUNK : (c + 1) * CHUNK]
                w1 = wts[1, k, :, c * CHUNK : (c + 1) * CHUNK]
                left = jnp.concatenate([jnp.where(high == jnp.bfloat16(h), w0, zero) for h in range(LEVELS)], axis=0)
                right = jnp.concatenate([jnp.where(low == jnp.bfloat16(l), w1, zero) for l in range(LEVELS)], axis=0)
                part_sum = lax.dot_general(left, right, (((1,), (1,)), ((), ())), preferred_element_type=jnp.float32)
                side = index % 2
                sums[side] = part_sum if sums[side] is None else sums[side] + part_sum
                index += 1
        joint = sums[0] + sums[1]
        own_row = lax.broadcasted_iota(jnp.int32, (GROUP, lanes), 0)
        own_col = lax.broadcasted_iota(jnp.int32, (GROUP, lanes), 1)
        keep = own_row == own_col % GROUP
        lines = []
        for h in range(LEVELS):
            lines.append(jnp.sum(jnp.where(keep, joint[h * GROUP : (h + 1) * GROUP], 0.0), axis=0, keepdims=True))
        return jnp.concatenate(lines, axis=0)

    def outgoing(step, e):
        target = ((team + e) % replicas) * groups + (seat + step) % groups
        slot = step * replicas + e
        return pltpu.make_async_remote_copy(
            src_ref=stage.at[step],
            dst_ref=inbox.at[slot],
            send_sem=send_sem.at[slot],
            recv_sem=recv_sem.at[slot],
            device_id={"rows": target},
            device_id_type=MESH,
        )

    def do_group(turn, carry):
        step = (turn + 1) % groups
        stage[step] = group_hist((seat + step) % groups)

        @pl.when(turn == 0)
        def _():
            pl.semaphore_wait(barrier, ranks - 1)

        @pl.when(turn < groups - 1)
        def _():
            for e in range(replicas):
                outgoing(step, e).start()

        return carry

    lax.fori_loop(0, groups, do_group, 0)
    for e in range(1, replicas):
        outgoing(0, e).start()

    total = stage[0]
    for step in range(groups):
        for e in range(replicas):
            if step + e > 0:
                outgoing(step, e).wait()
                total = total + inbox[step * replicas + e]

    src = lax.broadcasted_iota(jnp.int32, (lanes, lanes), 0)
    dst = lax.broadcasted_iota(jnp.int32, (lanes, lanes), 1)
    same = src % GROUP == dst % GROUP
    earlier = jnp.where(jnp.logical_and(same, src < dst), 1.0, 0.0).astype(jnp.bfloat16)
    every = jnp.where(same, 1.0, 0.0).astype(jnp.bfloat16)
    p0 = total.astype(jnp.bfloat16).astype(jnp.float32)
    p1 = (total - p0).astype(jnp.bfloat16).astype(jnp.float32)
    p2 = total - p0 - p1
    split = jnp.concatenate([p0, p1, p2], axis=0).astype(jnp.bfloat16)
    inner3 = jnp.dot(split, earlier, preferred_element_type=jnp.float32)
    level3 = jnp.dot(split, every, preferred_element_type=jnp.float32)
    inner = inner3[:LEVELS] + inner3[LEVELS : 2 * LEVELS] + inner3[2 * LEVELS :]
    level = level3[:LEVELS] + level3[LEVELS : 2 * LEVELS] + level3[2 * LEVELS :]
    inv = 1.0 / (total + 1.0)
    thr_load.wait()
    column = jnp.broadcast_to(thr_ref[...], (LANES, thr_ref.shape[1])).T
    whole = jnp.sum(level, axis=0, keepdims=True)
    target = column * whole[:, :LANES]
    run = jnp.zeros((1, lanes), jnp.float32)
    acc = jnp.zeros((thr_ref.shape[1], LANES), jnp.float32)
    for h in range(LEVELS):
        before = inner[h : h + 1] + run
        run = run + level[h : h + 1]
        for t in range(lanes // LANES):
            cut = slice(t * LANES, (t + 1) * LANES)
            ratio = (target - before[:, cut]) * inv[h : h + 1, cut]
            acc = acc + jnp.clip(ratio, 0.0, 1.0)
    turned = acc.T
    cuts = turned[:GROUP]
    for j in range(1, LANES // GROUP):
        cuts = cuts + turned[j * GROUP : (j + 1) * GROUP]
    mine[...] = cuts
    here = pl.multiple_of(seat * GROUP, GROUP)

    def spread(step):
        return pltpu.make_async_remote_copy(
            src_ref=mine,
            dst_ref=out_ref.at[pl.ds(here, GROUP), :],
            send_sem=gather_send.at[step],
            recv_sem=gather_recv.at[step],
            device_id={"rows": team * groups + (seat + step) % groups},
            device_id_type=MESH,
        )

    for step in range(1, groups):
        spread(step).start()
    out_ref[pl.ds(here, GROUP), :] = cuts
    for step in range(1, groups):
        spread(step).wait()


def solution(mesh):
    ranks = mesh.shape["rows"]

    def local(bins, hessian, thresholds):
        words, width = bins.shape
        groups = width // GROUP
        quantiles = thresholds.shape[0]
        lanes = LEVELS * GROUP
        return pl.pallas_call(
            functools.partial(kernel, ranks),
            out_shape=pltpu.VMEM((width, quantiles), jnp.float32),
            in_specs=[pl.BlockSpec(memory_space=pl.ANY)] * 3,
            out_specs=pl.BlockSpec(memory_space=pltpu.VMEM),
            scratch_shapes=[
                pltpu.VMEM((words, width), jnp.int32),
                pltpu.VMEM((4 * words // LANES, LANES), jnp.float32),
                pltpu.VMEM((1, quantiles), jnp.float32),
                pltpu.VMEM((width, words), jnp.int32),
                pltpu.VMEM((2, 4, GROUP, words), jnp.bfloat16),
                pltpu.VMEM((groups, LEVELS, lanes), jnp.float32),
                pltpu.VMEM((ranks, LEVELS, lanes), jnp.float32),
                pltpu.VMEM((GROUP, quantiles), jnp.float32),
                pltpu.SemaphoreType.DMA((words // LANES + 2,)),
                pltpu.SemaphoreType.DMA((ranks,)),
                pltpu.SemaphoreType.DMA((ranks,)),
                pltpu.SemaphoreType.DMA((groups,)),
                pltpu.SemaphoreType.DMA((groups,)),
            ],
            compiler_params=pltpu.CompilerParams(collective_id=0, has_side_effects=True),
        )(bins, hessian.reshape(-1, LANES), thresholds.reshape(1, -1))

    in_specs = (P("rows", "feat"), P("rows"), P())
    return jax.shard_map(local, mesh=mesh, in_specs=in_specs, out_specs=P("feat", None), check_vma=False)
```

```python
import functools

import jax
import jax.numpy as jnp
from jax import lax
from jax.experimental import pallas as pl
from jax.experimental.pallas import tpu as pltpu
from jax.sharding import PartitionSpec as P

BINS = 256
LEVELS = 16
GROUP = 16
LANES = 128
CHUNK = 256
MESH = pl.DeviceIdType.MESH


def kernel(ranks, bins_hbm, hess_hbm, thr_hbm, out_ref, bins_ref, hess_ref, thr_ref, prefix, column_ref, cols, wts, stage, inbox, mine, load_sem, send_sem, recv_sem, gather_send, gather_recv):
    words, width = bins_ref.shape
    tiles = words // LANES
    hess_load = pltpu.make_async_copy(hess_hbm, hess_ref, load_sem.at[tiles])
    hess_load.start()
    bins_loads = []
    for t in range(tiles):
        part = pl.ds(t * LANES, LANES)
        bins_loads.append(pltpu.make_async_copy(bins_hbm.at[part, :], bins_ref.at[part, :], load_sem.at[t]))
        bins_loads[t].start()
    thr_load = pltpu.make_async_copy(thr_hbm, thr_ref, load_sem.at[tiles + 1])
    thr_load.start()
    groups = width // GROUP
    replicas = ranks // groups
    lanes = LEVELS * GROUP
    me = lax.axis_index("rows")
    team, seat = me // groups, me % groups

    barrier = pltpu.get_barrier_semaphore()
    for step in range(1, ranks):
        pl.semaphore_signal(barrier, inc=1, device_id={"rows": (me + step) % ranks}, device_id_type=MESH)

    src = lax.broadcasted_iota(jnp.int32, (lanes, lanes), 0)
    dst = lax.broadcasted_iota(jnp.int32, (lanes, lanes), 1)
    gap = dst - src
    same = jnp.bitwise_and(gap, GROUP - 1) == 0
    prefix[:, :lanes] = jnp.where(jnp.logical_and(same, gap > 0), 1.0, 0.0).astype(jnp.bfloat16)
    prefix[:, lanes:] = jnp.where(same, 1.0, 0.0).astype(jnp.bfloat16)

    row = lax.broadcasted_iota(jnp.int32, (LANES, LANES), 0)
    col = lax.broadcasted_iota(jnp.int32, (LANES, LANES), 1)
    quarter = LANES // 4
    order = jnp.where(row == 4 * (col % quarter) + col // quarter, 1.0, 0.0).astype(jnp.bfloat16)
    lane = lax.broadcasted_iota(jnp.int32, (2 * tiles, LANES), 1) // quarter
    hess_load.wait()
    for t in range(tiles):
        bins_loads[t].wait()
    thr_load.wait()
    for t in range(tiles):
        cols[:, t * LANES : (t + 1) * LANES] = bins_ref[t * LANES : (t + 1) * LANES, :].T
    column_ref[...] = jnp.broadcast_to(thr_ref[...], (LANES, thr_ref.shape[1])).T
    flat = jnp.concatenate([hess_ref[pl.ds(j, tiles, stride=4), :] for j in range(4)], axis=0)
    left_factor = jnp.ones_like(flat)
    miss = jnp.abs(flat - flat.astype(jnp.bfloat16).astype(jnp.float32))
    for j in range(1, 128, 2):
        factor = 1.0 + j / 128.0
        other = (flat * (1.0 / factor)).astype(jnp.bfloat16).astype(jnp.float32)
        away = jnp.abs(flat - other * factor)
        left_factor = jnp.where(away < miss, factor, left_factor)
        miss = jnp.minimum(miss, away)
    right_factor = flat / left_factor
    pieces = jnp.concatenate([x[j * tiles : (j + 1) * tiles] for j in range(4) for x in (left_factor, right_factor)], axis=0)
    moved = jnp.dot(pieces.astype(jnp.bfloat16), order, preferred_element_type=jnp.float32)
    for k in range(4):
        plane = None
        for j in range(4):
            block = moved[2 * tiles * j : 2 * tiles * (j + 1)]
            if j != k:
                block = pltpu.roll(block, (quarter * (j - k)) % LANES, 1)
            plane = block if plane is None else jnp.where(lane == j, block, plane)
        for piece in range(2):
            for t in range(tiles):
                line = plane[piece * tiles + t : piece * tiles + t + 1]
                wts[piece, k, :, t * LANES : (t + 1) * LANES] = jnp.broadcast_to(line, (GROUP, LANES)).astype(jnp.bfloat16)

    def peer(step):
        place, bit = 0, 1
        while bit < groups:
            place = place + (seat // bit + step // bit) % 2 * bit
            bit *= 2
        return place

    def group_hist(group):
        base = pl.multiple_of(group * GROUP, GROUP)
        zero = jnp.zeros((GROUP, CHUNK), jnp.bfloat16)
        sums = [None, None]
        index = 0
        for c in range(words // CHUNK):
            part = cols[pl.ds(base, GROUP), c * CHUNK : (c + 1) * CHUNK]
            for k in range(4):
                high = jnp.bitwise_and(jnp.right_shift(part, 8 * k + 4), 15).astype(jnp.float32).astype(jnp.bfloat16)
                low = jnp.bitwise_and(jnp.right_shift(part, 8 * k), 15).astype(jnp.float32).astype(jnp.bfloat16)
                w0 = wts[0, k, :, c * CHUNK : (c + 1) * CHUNK]
                w1 = wts[1, k, :, c * CHUNK : (c + 1) * CHUNK]
                left = jnp.concatenate([jnp.where(high == jnp.bfloat16(h), w0, zero) for h in range(LEVELS)], axis=0)
                right = jnp.concatenate([jnp.where(low == jnp.bfloat16(l), w1, zero) for l in range(LEVELS)], axis=0)
                part_sum = lax.dot_general(left, right, (((1,), (1,)), ((), ())), preferred_element_type=jnp.float32)
                side = index % 2
                sums[side] = part_sum if sums[side] is None else sums[side] + part_sum
                index += 1
        joint = sums[0] + sums[1]
        own_row = lax.broadcasted_iota(jnp.int32, (GROUP, lanes), 0)
        own_col = lax.broadcasted_iota(jnp.int32, (GROUP, lanes), 1)
        keep = own_row == own_col % GROUP
        lines = []
        for h in range(LEVELS):
            lines.append(jnp.sum(jnp.where(keep, joint[h * GROUP : (h + 1) * GROUP], 0.0), axis=0, keepdims=True))
        return jnp.concatenate(lines, axis=0)

    def outgoing(step, e):
        target = ((team + e) % replicas) * groups + peer(step)
        slot = step * replicas + e
        return pltpu.make_async_remote_copy(
            src_ref=stage.at[step],
            dst_ref=inbox.at[slot],
            send_sem=send_sem.at[slot],
            recv_sem=recv_sem.at[slot],
            device_id={"rows": target},
            device_id_type=MESH,
        )

    def do_group(turn, carry):
        step = groups - 1 - turn
        stage[step] = group_hist(peer(step))

        @pl.when(turn == 0)
        def _():
            pl.semaphore_wait(barrier, ranks - 1)

        @pl.when(turn < groups - 1)
        def _():
            for e in range(replicas):
                outgoing(step, e).start()

        return carry

    lax.fori_loop(0, groups, do_group, 0)
    for e in range(1, replicas):
        outgoing(0, e).start()

    total = stage[0]
    for step in reversed(range(groups)):
        for e in range(replicas):
            if step + e > 0:
                outgoing(step, e).wait()
                total = total + inbox[step * replicas + e]

    p0 = total.astype(jnp.bfloat16).astype(jnp.float32)
    p1 = (total - p0).astype(jnp.bfloat16).astype(jnp.float32)
    p2 = total - p0 - p1
    split = jnp.concatenate([p0, p1, p2], axis=0).astype(jnp.bfloat16)
    sums3 = jnp.dot(split, prefix[...], preferred_element_type=jnp.float32)
    inner3, level3 = sums3[:, :lanes], sums3[:, lanes:]
    inner = inner3[:LEVELS] + inner3[LEVELS : 2 * LEVELS] + inner3[2 * LEVELS :]
    level = level3[:LEVELS] + level3[LEVELS : 2 * LEVELS] + level3[2 * LEVELS :]
    inv = 1.0 / (total + 1.0)
    whole = jnp.sum(level, axis=0, keepdims=True)
    target = column_ref[...] * whole[:, :LANES]
    run = jnp.zeros((1, lanes), jnp.float32)
    acc = jnp.zeros((thr_ref.shape[1], LANES), jnp.float32)
    for h in range(LEVELS):
        before = inner[h : h + 1] + run
        run = run + level[h : h + 1]
        for t in range(lanes // LANES):
            cut = slice(t * LANES, (t + 1) * LANES)
            ratio = (target - before[:, cut]) * inv[h : h + 1, cut]
            acc = acc + jnp.clip(ratio, 0.0, 1.0)
    turned = acc.T
    cuts = turned[:GROUP]
    for j in range(1, LANES // GROUP):
        cuts = cuts + turned[j * GROUP : (j + 1) * GROUP]
    mine[...] = cuts
    here = pl.multiple_of(seat * GROUP, GROUP)

    def spread(step):
        return pltpu.make_async_remote_copy(
            src_ref=mine,
            dst_ref=out_ref.at[pl.ds(here, GROUP), :],
            send_sem=gather_send.at[step],
            recv_sem=gather_recv.at[step],
            device_id={"rows": team * groups + peer(step)},
            device_id_type=MESH,
        )

    for step in reversed(range(1, groups)):
        spread(step).start()
    out_ref[pl.ds(here, GROUP), :] = cuts
    for step in range(1, groups):
        spread(step).wait()


def solution(mesh):
    ranks = mesh.shape["rows"]

    def local(bins, hessian, thresholds):
        words, width = bins.shape
        groups = width // GROUP
        quantiles = thresholds.shape[0]
        lanes = LEVELS * GROUP
        return pl.pallas_call(
            functools.partial(kernel, ranks),
            out_shape=pltpu.VMEM((width, quantiles), jnp.float32),
            in_specs=[pl.BlockSpec(memory_space=pl.ANY)] * 3,
            out_specs=pl.BlockSpec(memory_space=pltpu.VMEM),
            scratch_shapes=[
                pltpu.VMEM((words, width), jnp.int32),
                pltpu.VMEM((4 * words // LANES, LANES), jnp.float32),
                pltpu.VMEM((1, quantiles), jnp.float32),
                pltpu.VMEM((lanes, 2 * lanes), jnp.bfloat16),
                pltpu.VMEM((quantiles, LANES), jnp.float32),
                pltpu.VMEM((width, words), jnp.int32),
                pltpu.VMEM((2, 4, GROUP, words), jnp.bfloat16),
                pltpu.VMEM((groups, LEVELS, lanes), jnp.float32),
                pltpu.VMEM((ranks, LEVELS, lanes), jnp.float32),
                pltpu.VMEM((GROUP, quantiles), jnp.float32),
                pltpu.SemaphoreType.DMA((words // LANES + 2,)),
                pltpu.SemaphoreType.DMA((ranks,)),
                pltpu.SemaphoreType.DMA((ranks,)),
                pltpu.SemaphoreType.DMA((groups,)),
                pltpu.SemaphoreType.DMA((groups,)),
            ],
            compiler_params=pltpu.CompilerParams(collective_id=0, has_side_effects=True),
        )(bins, hessian.reshape(-1, LANES), thresholds.reshape(1, -1))

    in_specs = (P("rows", "feat"), P("rows"), P())
    return jax.shard_map(local, mesh=mesh, in_specs=in_specs, out_specs=P("feat", None), check_vma=False)
```

```python
import functools

import jax
import jax.numpy as jnp
from jax import lax
from jax.experimental import pallas as pl
from jax.experimental.pallas import tpu as pltpu
from jax.sharding import PartitionSpec as P

BINS = 256
LEVELS = 16
GROUP = 16
LANES = 128
CHUNK = 256
MESH = pl.DeviceIdType.MESH


def kernel(ranks, bins_hbm, hess_hbm, thr_hbm, out_ref, bins_ref, hess_ref, thr_ref, prefix, column_ref, cols, wts, stage, inbox, mine, load_sem, send_sem, recv_sem, gather_send, gather_recv):
    words, width = bins_ref.shape
    tiles = words // LANES
    hess_load = pltpu.make_async_copy(hess_hbm, hess_ref, load_sem.at[tiles])
    hess_load.start()
    bins_loads = []
    for t in range(tiles):
        part = pl.ds(t * LANES, LANES)
        bins_loads.append(pltpu.make_async_copy(bins_hbm.at[part, :], bins_ref.at[part, :], load_sem.at[t]))
        bins_loads[t].start()
    thr_load = pltpu.make_async_copy(thr_hbm, thr_ref, load_sem.at[tiles + 1])
    thr_load.start()
    groups = width // GROUP
    replicas = ranks // groups
    lanes = LEVELS * GROUP
    me = lax.axis_index("rows")
    team, seat = me // groups, me % groups

    barrier = pltpu.get_barrier_semaphore()
    for step in range(1, ranks):
        pl.semaphore_signal(barrier, inc=1, device_id={"rows": (me + step) % ranks}, device_id_type=MESH)

    src = lax.broadcasted_iota(jnp.int32, (lanes, lanes), 0)
    dst = lax.broadcasted_iota(jnp.int32, (lanes, lanes), 1)
    gap = dst - src
    same = jnp.bitwise_and(gap, GROUP - 1) == 0
    prefix[:, :lanes] = jnp.where(jnp.logical_and(same, gap > 0), 1.0, 0.0).astype(jnp.bfloat16)
    prefix[:, lanes:] = jnp.where(same, 1.0, 0.0).astype(jnp.bfloat16)

    row = lax.broadcasted_iota(jnp.int32, (LANES, LANES), 0)
    col = lax.broadcasted_iota(jnp.int32, (LANES, LANES), 1)
    quarter = LANES // 4
    order = jnp.where(row == 4 * (col % quarter) + col // quarter, 1.0, 0.0).astype(jnp.bfloat16)
    lane = lax.broadcasted_iota(jnp.int32, (2 * tiles, LANES), 1) // quarter
    hess_load.wait()
    flat = jnp.concatenate([hess_ref[pl.ds(j, tiles, stride=4), :] for j in range(4)], axis=0)
    left_factor = jnp.ones_like(flat)
    miss = jnp.abs(flat - flat.astype(jnp.bfloat16).astype(jnp.float32))
    for j in range(1, 128, 2):
        factor = 1.0 + j / 128.0
        other = (flat * (1.0 / factor)).astype(jnp.bfloat16).astype(jnp.float32)
        away = jnp.abs(flat - other * factor)
        left_factor = jnp.where(away < miss, factor, left_factor)
        miss = jnp.minimum(miss, away)
    right_factor = flat / left_factor
    for t in range(tiles):
        bins_loads[t].wait()
    thr_load.wait()
    for t in range(tiles):
        cols[:, t * LANES : (t + 1) * LANES] = bins_ref[t * LANES : (t + 1) * LANES, :].T
    column_ref[...] = jnp.broadcast_to(thr_ref[...], (LANES, thr_ref.shape[1])).T
    pieces = jnp.concatenate([x[j * tiles : (j + 1) * tiles] for j in range(4) for x in (left_factor, right_factor)], axis=0)
    moved = jnp.dot(pieces.astype(jnp.bfloat16), order, preferred_element_type=jnp.float32)
    for k in range(4):
        plane = None
        for j in range(4):
            block = moved[2 * tiles * j : 2 * tiles * (j + 1)]
            if j != k:
                block = pltpu.roll(block, (quarter * (j - k)) % LANES, 1)
            plane = block if plane is None else jnp.where(lane == j, block, plane)
        for piece in range(2):
            for t in range(tiles):
                line = plane[piece * tiles + t : piece * tiles + t + 1]
                wts[piece, k, :, t * LANES : (t + 1) * LANES] = jnp.broadcast_to(line, (GROUP, LANES)).astype(jnp.bfloat16)

    def peer(step):
        place, bit = 0, 1
        while bit < groups:
            place = place + (seat // bit + step // bit) % 2 * bit
            bit *= 2
        return place

    def group_hist(group):
        base = pl.multiple_of(group * GROUP, GROUP)
        zero = jnp.zeros((GROUP, CHUNK), jnp.bfloat16)
        sums = [None, None]
        index = 0
        for c in range(words // CHUNK):
            part = cols[pl.ds(base, GROUP), c * CHUNK : (c + 1) * CHUNK]
            for k in range(4):
                high = jnp.bitwise_and(jnp.right_shift(part, 8 * k + 4), 15).astype(jnp.float32).astype(jnp.bfloat16)
                low = jnp.bitwise_and(jnp.right_shift(part, 8 * k), 15).astype(jnp.float32).astype(jnp.bfloat16)
                w0 = wts[0, k, :, c * CHUNK : (c + 1) * CHUNK]
                w1 = wts[1, k, :, c * CHUNK : (c + 1) * CHUNK]
                left = jnp.concatenate([jnp.where(high == jnp.bfloat16(h), w0, zero) for h in range(LEVELS)], axis=0)
                right = jnp.concatenate([jnp.where(low == jnp.bfloat16(l), w1, zero) for l in range(LEVELS)], axis=0)
                part_sum = lax.dot_general(left, right, (((1,), (1,)), ((), ())), preferred_element_type=jnp.float32)
                side = index % 2
                sums[side] = part_sum if sums[side] is None else sums[side] + part_sum
                index += 1
        joint = sums[0] + sums[1]
        own_row = lax.broadcasted_iota(jnp.int32, (GROUP, lanes), 0)
        own_col = lax.broadcasted_iota(jnp.int32, (GROUP, lanes), 1)
        keep = own_row == own_col % GROUP
        lines = []
        for h in range(LEVELS):
            lines.append(jnp.sum(jnp.where(keep, joint[h * GROUP : (h + 1) * GROUP], 0.0), axis=0, keepdims=True))
        return jnp.concatenate(lines, axis=0)

    def outgoing(step, e):
        target = ((team + e) % replicas) * groups + peer(step)
        slot = step * replicas + e
        return pltpu.make_async_remote_copy(
            src_ref=stage.at[step],
            dst_ref=inbox.at[slot],
            send_sem=send_sem.at[slot],
            recv_sem=recv_sem.at[slot],
            device_id={"rows": target},
            device_id_type=MESH,
        )

    def do_pair(turn, carry):
        step = groups - 1 - 2 * turn
        first = group_hist(peer(step))
        second = group_hist(peer(step - 1))
        stage[step] = first
        stage[step - 1] = second

        @pl.when(turn == 0)
        def _():
            pl.semaphore_wait(barrier, ranks - 1)

        for e in range(replicas):
            outgoing(step, e).start()

        @pl.when(turn < groups // 2 - 1)
        def _():
            for e in range(replicas):
                outgoing(step - 1, e).start()

        return carry

    lax.fori_loop(0, groups // 2, do_pair, 0)
    for e in range(1, replicas):
        outgoing(0, e).start()

    total = stage[0]
    for step in reversed(range(groups)):
        for e in range(replicas):
            if step + e > 0:
                outgoing(step, e).wait()
                total = total + inbox[step * replicas + e]

    p0 = total.astype(jnp.bfloat16).astype(jnp.float32)
    p1 = (total - p0).astype(jnp.bfloat16).astype(jnp.float32)
    p2 = total - p0 - p1
    split = jnp.concatenate([p0, p1, p2], axis=0).astype(jnp.bfloat16)
    sums3 = jnp.dot(split, prefix[...], preferred_element_type=jnp.float32)
    inner3, level3 = sums3[:, :lanes], sums3[:, lanes:]
    inner = inner3[:LEVELS] + inner3[LEVELS : 2 * LEVELS] + inner3[2 * LEVELS :]
    level = level3[:LEVELS] + level3[LEVELS : 2 * LEVELS] + level3[2 * LEVELS :]
    inv = 1.0 / (total + 1.0)
    whole = jnp.sum(level, axis=0, keepdims=True)
    target = column_ref[...] * whole[:, :LANES]
    run = jnp.zeros((1, lanes), jnp.float32)
    acc = jnp.zeros((thr_ref.shape[1], LANES), jnp.float32)
    for h in range(LEVELS):
        before = inner[h : h + 1] + run
        run = run + level[h : h + 1]
        for t in range(lanes // LANES):
            cut = slice(t * LANES, (t + 1) * LANES)
            ratio = (target - before[:, cut]) * inv[h : h + 1, cut]
            acc = acc + jnp.clip(ratio, 0.0, 1.0)
    turned = acc.T
    cuts = turned[:GROUP]
    for j in range(1, LANES // GROUP):
        cuts = cuts + turned[j * GROUP : (j + 1) * GROUP]
    mine[...] = cuts
    here = pl.multiple_of(seat * GROUP, GROUP)

    def spread(step):
        return pltpu.make_async_remote_copy(
            src_ref=mine,
            dst_ref=out_ref.at[pl.ds(here, GROUP), :],
            send_sem=gather_send.at[step],
            recv_sem=gather_recv.at[step],
            device_id={"rows": team * groups + peer(step)},
            device_id_type=MESH,
        )

    for step in reversed(range(1, groups)):
        spread(step).start()
    out_ref[pl.ds(here, GROUP), :] = cuts
    for step in range(1, groups):
        spread(step).wait()


def solution(mesh):
    ranks = mesh.shape["rows"]

    def local(bins, hessian, thresholds):
        words, width = bins.shape
        groups = width // GROUP
        quantiles = thresholds.shape[0]
        lanes = LEVELS * GROUP
        return pl.pallas_call(
            functools.partial(kernel, ranks),
            out_shape=pltpu.VMEM((width, quantiles), jnp.float32),
            in_specs=[pl.BlockSpec(memory_space=pl.ANY)] * 3,
            out_specs=pl.BlockSpec(memory_space=pltpu.VMEM),
            scratch_shapes=[
                pltpu.VMEM((words, width), jnp.int32),
                pltpu.VMEM((4 * words // LANES, LANES), jnp.float32),
                pltpu.VMEM((1, quantiles), jnp.float32),
                pltpu.VMEM((lanes, 2 * lanes), jnp.bfloat16),
                pltpu.VMEM((quantiles, LANES), jnp.float32),
                pltpu.VMEM((width, words), jnp.int32),
                pltpu.VMEM((2, 4, GROUP, words), jnp.bfloat16),
                pltpu.VMEM((groups, LEVELS, lanes), jnp.float32),
                pltpu.VMEM((ranks, LEVELS, lanes), jnp.float32),
                pltpu.VMEM((GROUP, quantiles), jnp.float32),
                pltpu.SemaphoreType.DMA((words // LANES + 2,)),
                pltpu.SemaphoreType.DMA((ranks,)),
                pltpu.SemaphoreType.DMA((ranks,)),
                pltpu.SemaphoreType.DMA((groups,)),
                pltpu.SemaphoreType.DMA((groups,)),
            ],
            compiler_params=pltpu.CompilerParams(collective_id=0, has_side_effects=True),
        )(bins, hessian.reshape(-1, LANES), thresholds.reshape(1, -1))

    in_specs = (P("rows", "feat"), P("rows"), P())
    return jax.shard_map(local, mesh=mesh, in_specs=in_specs, out_specs=P("feat", None), check_vma=False)
```
